32 devices in a mesh: orb: 4 (over y, x), aux: 8 (over z, core).
Axes of the slice: x: 2, y: 2, z: 4, core: 2. Of those that a mesh axis runs over, the one named last changes fastest.
Arguments:
- raw_rows: bfloat16 [128, 1024, 128], P('orb', 'aux'), may hold values from -4 to 4
- fit_metric: bfloat16 [128, 512, 512], P(('orb', 'aux'))
- domain: int32 [128, 512], P('orb'), may hold values from 0 to 127, as said below
- counts: int32 [128, 8], P('orb'), may hold values from 32 to 128, as said below
- orbital_ids: int32 [128], P(('orb', 'aux')), may hold values from 0 to 127, each once
- occ_energy: float32 [128], replicated, may hold values from -1.5 to -0.3
- osv_energy: bfloat16 [128, 128], P(('orb', 'aux')), may hold values from 0.29882812 to 3
- matchings: int32 [4, 4], replicated, may hold values from 0 to 3, as said below
- screening: int32 [128, 5, 4], P(('orb', 'aux')), may hold values 0 or 1
Outputs:
- density: float32 [128, 1024, 128], P('orb', 'aux')
- pair_energy: float32 [128, 5, 4], P(('orb', 'aux'))
The draws below stay inside these ranges and needn't reach their ends.
Inputs may be any that keep to these rules, and one draw needn't show every extreme that they name: `counts`: every row sums to 512; every entry is at most 128, and every row has an entry equal to 128. `domain`: the positions of a row are taken by owner 0 first, then owner 1 and so on, in the numbers that counts gives; within one owner's run the entries are distinct. `matchings`: row q maps orb index o to o XOR m_q, with a mask m_q from 1 to 3; rounds may repeat a mask.
All inputs are finite; a program needn't handle non-finite values. No bound on the sum of `screening` on one device may be relied on, other than what follows from the above.
Results may differ from the reference program's by a relative error of at most 0.0029.
Values may be sent and summed in bfloat16 or wider, within the bound.
A program may use at most 128 MiB of HBM per device.

```python
import math
import jax
import jax.numpy as jnp
from jax import lax

NOSV = 128
NFIT = 512
OCC_DEV = 4
AUX_DEV = 128
MATCHES = 4
NOCC = 128
NAUX = 1024
CAP = 128
N_ORB = 4
N_AUX = 8
DEVICES = 32


def domain_tables(key):
    key = jax.random.fold_in(key, 5)
    key_owner, key_second, key_extra, key_rows = jax.random.split(key, 4)
    base = NFIT // (2 * N_AUX)
    extra = CAP - base
    spare = NFIT - N_AUX * base - extra
    owner = jnp.minimum(jax.random.randint(key_owner, (NOCC,), 0, N_AUX), jax.random.randint(key_second, (NOCC,), 0, N_AUX)).astype(jnp.int32)
    slots_total = (N_AUX - 1) * extra
    orders = jax.vmap(lambda single: jax.random.permutation(single, slots_total))(jax.random.split(key_extra, NOCC))
    taken = (orders < spare).astype(jnp.int32).reshape(NOCC, N_AUX - 1, extra).sum(axis=2)
    owners = jnp.arange(N_AUX, dtype=jnp.int32)
    ordinal = jnp.clip(owners[None, :] - (owners[None, :] > owner[:, None]).astype(jnp.int32), 0, N_AUX - 2)
    others = jnp.take_along_axis(taken, ordinal, axis=1)
    counts = (base + jnp.where(owners[None, :] == owner[:, None], extra, others)).astype(jnp.int32)
    row_orders = jax.vmap(lambda single: jax.random.permutation(single, AUX_DEV))(jax.random.split(key_rows, NOCC * N_AUX))
    row_orders = row_orders.reshape(NOCC, N_AUX * AUX_DEV).astype(jnp.int32)
    run_ends = jnp.cumsum(counts, axis=1)
    run_starts = run_ends - counts
    positions = jnp.arange(NFIT, dtype=jnp.int32)
    which = jnp.sum((positions[None, :, None] >= run_ends[:, None, :]).astype(jnp.int32), axis=2)
    offset = positions[None, :] - jnp.take_along_axis(run_starts, which, axis=1)
    domain = jnp.take_along_axis(row_orders, which * AUX_DEV + offset, axis=1)
    return (counts, domain.astype(jnp.int32))


def draw_counts(key, part):
    return domain_tables(key)[0]


def draw_domain(key, part):
    return domain_tables(key)[1]


def draw_matchings(key, part):
    key = jax.random.fold_in(key, 17)
    masks = jax.random.randint(key, (MATCHES,), 1, N_ORB).astype(jnp.int32)
    indices = jnp.arange(N_ORB, dtype=jnp.int32)
    return jnp.bitwise_xor(indices[None, :], masks[:, None]).astype(jnp.int32)


def draw_fit_metric(key, part):
    key = jax.random.fold_in(key, 11)
    key_off, key_diag = jax.random.split(key)
    off = jax.random.normal(key_off, (NOCC, NFIT, NFIT), jnp.float32) * (0.5 / math.sqrt(NFIT))
    diag = jax.random.uniform(key_diag, (NOCC, NFIT), jnp.float32, 0.5, 2.0)
    indices = jnp.arange(NFIT, dtype=jnp.int32)
    on_diag = indices[:, None] == indices[None, :]
    return jnp.where(on_diag[None, :, :], diag[:, :, None], off).astype(jnp.bfloat16)


def with_ends(entries, stream_key, smallest, high):
    longest = entries.shape.index(max(entries.shape))
    spots = []
    for shift in (0, 1):
        where = [jax.random.randint(jax.random.fold_in(stream_key, axis), (), 0, length) for axis, length in enumerate(entries.shape)]
        where[longest] = (where[longest] + shift) % entries.shape[longest]
        spots.append(tuple(where))
    return entries.at[spots[0]].set(smallest).at[spots[1]].set(high)


def level_of(rng, dims, cuts, smallest, largest):
    def one(axis_at, blocks):
        steps = jax.random.uniform(jax.random.fold_in(jax.random.fold_in(rng, 6), axis_at), (blocks,), jnp.float32, smallest / len(cuts), largest / len(cuts))
        return jnp.repeat(jnp.exp(steps), dims[axis_at] // blocks).reshape((-1,) + (1,) * (len(dims) - axis_at - 1))

    factor_of = one(*cuts[0])
    for cut in cuts[1:]:
        factor_of = factor_of * one(*cut)
    return factor_of


def noise(stream_key, shape, width, most, cuts=(), kind=jnp.bfloat16):
    drawn = jax.random.normal(stream_key, shape, jnp.float32) * width
    if len(cuts) > 0:
        drawn = level_of(stream_key, shape, cuts, -0.22, 0.18) * drawn
    return jnp.clip(drawn, min=-most, max=most).astype(kind)


def setup_inputs(seed: int = 0) -> dict:
    arg_keys = jax.random.split(jax.random.key(seed), 10)
    raw_rows = noise(arg_keys[0], (NOCC, NAUX, NOSV), (NAUX ** 0.25 / NFIT ** 0.5), 4.0, ((0, 4), (1, 8)))
    fit_metric = draw_fit_metric(jax.random.fold_in(arg_keys[9], 71), 0)
    domain = draw_domain(jax.random.fold_in(arg_keys[9], 71), 0)
    counts = draw_counts(jax.random.fold_in(arg_keys[9], 71), 0)
    orbital_ids = jax.random.permutation(arg_keys[4], NOCC).astype(jnp.int32)
    occ_energy = jnp.clip(jax.random.uniform(arg_keys[5], (NOCC,), jnp.float32, -1.5, -0.3), -1.5, -0.3)
    osv_energy = jnp.clip(jnp.exp(math.log(3.0) - 2.306499 * jax.random.uniform(arg_keys[6], (NOCC, NOSV), jnp.float32) ** level_of(arg_keys[6], (NOCC, NOSV), ((0, 32),), -0.2, 0.2)), 0.29882812, 3.0).astype(jnp.bfloat16)
    matchings = draw_matchings(jax.random.fold_in(arg_keys[9], 71), 0)
    screening = with_ends((jax.random.randint(arg_keys[8], (NOCC, MATCHES + 1, OCC_DEV), 0, 4) < 3).astype(jnp.int32), jax.random.fold_in(arg_keys[8], 1), 0, 1)
    return dict(raw_rows=raw_rows, fit_metric=fit_metric, domain=domain, counts=counts, orbital_ids=orbital_ids, occ_energy=occ_energy, osv_energy=osv_energy, matchings=matchings, screening=screening)


PAIR_SCALE = 1.3


def fit_one(operands):
    return jnp.dot(operands[0], operands[1], preferred_element_type=jnp.float32).astype(jnp.bfloat16)


def reference(raw_rows, fit_metric, domain, counts, orbital_ids, occ_energy, osv_energy, matchings, screening):
    run_ends = jnp.cumsum(counts, axis=1)
    positions = jnp.arange(NFIT, dtype=jnp.int32)
    source = jnp.sum((positions[None, :, None] >= run_ends[:, None, :]).astype(jnp.int32), axis=2)
    rows_global = (source * AUX_DEV + domain).astype(jnp.int32)
    slots_all = jnp.arange(NOCC, dtype=jnp.int32)
    gathered_rows = raw_rows[slots_all[:, None], rows_global]
    fitted = lax.map(fit_one, (fit_metric, gathered_rows))
    occ_values = occ_energy[orbital_ids]
    osv_values = osv_energy.astype(jnp.float32)
    local_range = jnp.arange(OCC_DEV, dtype=jnp.int32)

    def device_work(device):
        orb_index = device // N_AUX
        aux_index = device % N_AUX
        own_slots = device * OCC_DEV + local_range
        raw_full = jnp.zeros((OCC_DEV, NAUX, NOSV), jnp.bfloat16)
        raw_full = raw_full.at[local_range[:, None], rows_global[own_slots]].set(gathered_rows[own_slots])
        partner_devices = jnp.concatenate([device[None], (matchings[:, orb_index] * N_AUX + aux_index).astype(jnp.int32)])
        density = jnp.zeros((OCC_DEV, NAUX, NOSV), jnp.float32)
        energies = []
        for round_index in range(MATCHES + 1):
            partner_slots = partner_devices[round_index] * OCC_DEV + local_range
            far_fitted = fitted[partner_slots].astype(jnp.float32)
            far_rows = rows_global[partner_slots].reshape(-1)
            picked = raw_full[:, far_rows].reshape(OCC_DEV, OCC_DEV, NFIT, NOSV).astype(jnp.float32)
            integrals = jnp.einsum("klpa,lpb->klab", picked, far_fitted)
            denominator = (osv_values[own_slots][:, None, :, None] + osv_values[partner_slots][None, :, None, :]
                           - occ_values[own_slots][:, None, None, None] - occ_values[partner_slots][None, :, None, None])
            screen_round = screening[own_slots, round_index].astype(jnp.float32)
            amplitudes = (screen_round[:, :, None, None] * integrals / denominator).astype(jnp.bfloat16)
            amplitudes = lax.optimization_barrier(amplitudes).astype(jnp.float32)
            energies.append(PAIR_SCALE * jnp.sum(amplitudes * integrals, axis=(2, 3)) / (NOSV * NOSV))
            pieces = jnp.einsum("klab,lpb->klpa", amplitudes, far_fitted)
            density = density.at[:, far_rows].add(pieces.reshape(OCC_DEV, OCC_DEV * NFIT, NOSV))
        return density, jnp.stack(energies, axis=1)

    density, energies = lax.map(device_work, jnp.arange(DEVICES, dtype=jnp.int32))
    return density.reshape(NOCC, NAUX, NOSV), energies.reshape(NOCC, MATCHES + 1, OCC_DEV)
```

```python
import functools

import jax
import jax.numpy as jnp
from jax import lax
from jax.experimental import pallas as pl
from jax.experimental.pallas import tpu as pltpu
from jax.sharding import PartitionSpec as P

PAIR_SCALE = 1.3
MESH = pl.DeviceIdType.MESH
NT = (((1,), (1,)), ((), ()))


def kernel(
    n_orb,
    n_aux,
    raw_ref,
    metric_ref,
    domain_ref,
    counts_ref,
    ids_ref,
    occ_ref,
    osv_ref,
    match_ref,
    screen_ref,
    out_ref,
    energy_ref,
    raw_full,
    metric,
    st_own,
    st_far,
    ms,
    mask,
    rt,
    fitted,
    rows,
    levels,
    level_col,
    grid_full,
    integrals,
    amps,
    outgoing,
    raw_send,
    raw_recv,
    fit_send,
    fit_recv,
    meta_send,
    meta_recv,
    den_send,
    den_recv,
    local_sem,
):
    occ, fit = metric_ref.shape[0], metric_ref.shape[1]
    aux_dev, osv = raw_ref.shape[2], raw_ref.shape[3]
    aux_total = n_aux * aux_dev
    matches = match_ref.shape[0] // n_orb
    my_orb = lax.axis_index("orb")
    me = lax.axis_index("aux")

    def aux_peer(step):
        return lax.rem(me + step, n_aux)

    def orb_peer(step):
        return lax.rem(my_orb + step, n_orb)

    barrier = pltpu.get_barrier_semaphore()
    for step in range(1, n_aux):
        pl.semaphore_signal(barrier, inc=1, device_id=(my_orb, aux_peer(step)), device_id_type=MESH)
    for step in range(1, n_orb):
        pl.semaphore_signal(barrier, inc=1, device_id=(orb_peer(step), me), device_id_type=MESH)

    metric_copy = pltpu.make_async_copy(metric_ref, metric, local_sem.at[0])
    metric_copy.start()
    own_raw = pltpu.make_async_copy(raw_ref.at[me], raw_full.at[:, me], local_sem.at[1])
    own_raw.start()
    pl.semaphore_wait(barrier, n_aux + n_orb - 2)

    def raw_copy(k, step):
        return pltpu.make_async_remote_copy(
            src_ref=raw_ref.at[aux_peer(step), k],
            dst_ref=raw_full.at[k, me],
            send_sem=raw_send.at[k, step],
            recv_sem=raw_recv.at[k, step],
            device_id=(my_orb, aux_peer(step)),
            device_id_type=MESH,
        )

    def fit_copy(k, step):
        return pltpu.make_async_remote_copy(
            src_ref=fitted.at[k, 0],
            dst_ref=fitted.at[k, step],
            send_sem=fit_send.at[k, step],
            recv_sem=fit_recv.at[k, step],
            device_id=(orb_peer(step), me),
            device_id_type=MESH,
        )

    def meta_copy(which, ref, step):
        return pltpu.make_async_remote_copy(
            src_ref=ref.at[0],
            dst_ref=ref.at[step],
            send_sem=meta_send.at[which, step],
            recv_sem=meta_recv.at[which, step],
            device_id=(orb_peer(step), me),
            device_id_type=MESH,
        )

    def den_copy(owner):
        return pltpu.make_async_remote_copy(
            src_ref=outgoing.at[owner],
            dst_ref=out_ref.at[me],
            send_sem=den_send.at[owner],
            recv_sem=den_recv.at[lax.rem(me - owner + n_aux, n_aux)],
            device_id=(my_orb, owner),
            device_id_type=MESH,
        )

    def send_raw(k, carry):
        def one(step, inner):
            raw_copy(k, step).start()
            return inner

        return lax.fori_loop(1, n_aux, one, carry)

    lax.fori_loop(0, occ, send_raw, 0)

    positions = lax.broadcasted_iota(jnp.int32, (1, fit), 1)
    for k in range(occ):
        end = jnp.int32(0)
        owner = jnp.zeros((1, fit), jnp.int32)
        for j in range(n_aux):
            end = end + counts_ref[(me * occ + k) * n_aux + j]
            owner = owner + jnp.where(positions >= end, 1, 0)
        rows[0, k : k + 1, :] = owner * aux_dev + domain_ref[me, k : k + 1, :]
        level = osv_ref[k : k + 1, :].astype(jnp.float32) - occ_ref[ids_ref[k]]
        levels[0, k : k + 1, :] = level
        level_col[k * osv : (k + 1) * osv, :] = jnp.broadcast_to(level, (osv, osv)).T
    for step in range(1, n_orb):
        meta_copy(0, rows, step).start()
        meta_copy(1, levels, step).start()

    def place(row, target):
        height = 128
        base = lax.broadcasted_iota(jnp.int32, (height, fit), 0)
        for j in range(aux_total // height):
            target[j * height : (j + 1) * height, :] = jnp.where(
                base == row - j * height, 1.0, 0.0
            ).astype(jnp.bfloat16)

    metric_copy.wait()
    ones = jnp.ones((8, fit), jnp.bfloat16)

    def prepare(k, carry):
        place(rows[0, pl.ds(k, 1), :], st_own.at[k])
        ms[k] = lax.dot_general(
            metric[k], st_own[k], NT, preferred_element_type=jnp.float32
        ).astype(jnp.bfloat16)
        mask[k] = lax.dot_general(ones, st_own[k], NT, preferred_element_type=jnp.float32)
        return carry

    lax.fori_loop(0, occ, prepare, 0)
    own_raw.wait()

    def lanes(l, step):
        return pl.ds(pl.multiple_of((l * n_orb + step) * osv, osv), osv)

    def fit_own(k, carry):
        def arrived(step, inner):
            raw_copy(k, step).wait_recv()
            return inner

        lax.fori_loop(1, n_aux, arrived, 0)
        dense = raw_full[k].reshape(aux_total, osv)
        block = jnp.dot(ms[k], dense, preferred_element_type=jnp.float32).astype(jnp.bfloat16)
        fitted[k, 0] = block
        for step in range(1, n_orb):
            fit_copy(k, step).start()
        rt[pl.ds(pl.multiple_of(k * osv, osv), osv), :] = jnp.where(
            mask[k, 0:1, :] > 0.5, dense.astype(jnp.float32).T, 0.0
        ).astype(jnp.bfloat16)
        grid_full[:, lanes(k, 0)] = jnp.dot(
            st_own[k], block, preferred_element_type=jnp.float32
        ).astype(jnp.bfloat16)
        return carry

    lax.fori_loop(0, occ, fit_own, 0)

    for step in range(1, n_orb):
        meta_copy(0, rows, step).wait_recv()
        meta_copy(1, levels, step).wait_recv()

    def partners(l, carry):
        def spread(step, inner):
            place(rows[step, pl.ds(l, 1), :], st_far)
            fit_copy(l, step).wait_recv()
            grid_full[:, lanes(l, step)] = jnp.dot(
                st_far[...], fitted[l, step], preferred_element_type=jnp.float32
            ).astype(jnp.bfloat16)
            return inner

        lax.fori_loop(1, n_orb, spread, 0)
        wide = n_orb * osv
        part = pl.ds(pl.multiple_of(l * wide, wide), wide)
        integrals[...] = jnp.dot(rt[...], grid_full[:, part], preferred_element_type=jnp.float32)

        def terms(step, inner):
            far = levels[step, pl.ds(l, 1), :]
            peer = lax.rem(my_orb - step + n_orb, n_orb)
            local = pl.ds(pl.multiple_of(step * osv, osv), osv)
            for k in range(occ):
                base = k * (matches + 1) * occ
                weight = jnp.where(step == 0, screen_ref[base + l], 0)
                for q in range(matches):
                    weight = weight + jnp.where(
                        jnp.logical_and(step > 0, match_ref[q * n_orb + my_orb] == peer),
                        screen_ref[base + (q + 1) * occ + l],
                        0,
                    )
                value = integrals[k * osv : (k + 1) * osv, local]
                bottom = level_col[k * osv : (k + 1) * osv, :] + far
                amp = (value / bottom).astype(jnp.bfloat16).astype(jnp.float32)
                energy_ref[l, step, k : k + 1, :] = jnp.sum(amp * value, axis=0, keepdims=True)
                amps[k * osv : (k + 1) * osv, lanes(l, step)] = (
                    amp * weight.astype(jnp.float32)
                ).astype(jnp.bfloat16)
            return inner

        return lax.fori_loop(0, n_orb, terms, carry)

    lax.fori_loop(0, occ, partners, 0)

    pair = 2
    my_pair = me // pair

    def density(which):
        height = pair * aux_dev
        part = grid_full[pl.ds(pl.multiple_of(which * height, height), height), :]
        found = lax.dot_general(part, amps[...], NT, preferred_element_type=jnp.float32)
        found = found.astype(jnp.bfloat16)
        for c in range(pair):
            for k in range(occ):
                outgoing[which * pair + c, k] = found[
                    c * aux_dev : (c + 1) * aux_dev, k * osv : (k + 1) * osv
                ]

    def far_density(step, carry):
        which = lax.rem(my_pair + step, n_aux // pair)
        density(which)
        for c in range(pair):
            den_copy(which * pair + c).start()
        return carry

    lax.fori_loop(1, n_aux // pair, far_density, 0)
    density(my_pair)
    buddy = my_pair * pair + 1 - lax.rem(me, pair)
    den_copy(buddy).start()
    own_out = pltpu.make_async_copy(outgoing.at[me], out_ref.at[me], local_sem.at[2])
    own_out.start()

    def drain_raw(k, carry):
        def one(step, inner):
            raw_copy(k, step).wait_send()
            return inner

        lax.fori_loop(1, n_aux, one, 0)

        def two(step, inner):
            fit_copy(k, step).wait_send()
            return inner

        return lax.fori_loop(1, n_orb, two, carry)

    lax.fori_loop(0, occ, drain_raw, 0)
    for step in range(1, n_orb):
        meta_copy(0, rows, step).wait_send()
        meta_copy(1, levels, step).wait_send()

    def drain_density(step, carry):
        copy = den_copy(aux_peer(step))
        copy.wait_send()
        copy.wait_recv()
        return carry

    lax.fori_loop(1, n_aux, drain_density, 0)
    own_out.wait()


def per_device(
    raw_rows, fit_metric, domain, counts, orbital_ids, occ_energy, osv_energy, matchings, screening
):
    n_aux = lax.axis_size("aux")
    n_orb = lax.axis_size("orb")
    my_orb = lax.axis_index("orb")
    group_slots, aux_dev, osv = raw_rows.shape
    occ = group_slots // n_aux
    fit = domain.shape[1]
    aux_total = aux_dev * n_aux
    matches = matchings.shape[0]
    bf16, f32 = jnp.bfloat16, jnp.float32
    anywhere = pl.BlockSpec(memory_space=pl.ANY)
    vmem = pl.BlockSpec(memory_space=pltpu.VMEM)
    smem = pl.BlockSpec(memory_space=pltpu.SMEM)
    dma = pltpu.SemaphoreType.DMA
    returned, sums = pl.pallas_call(
        functools.partial(kernel, n_orb, n_aux),
        out_shape=(
            jax.ShapeDtypeStruct((n_aux, occ, aux_dev, osv), bf16),
            jax.ShapeDtypeStruct((occ, n_orb, occ, osv), f32),
        ),
        in_specs=[anywhere, anywhere, vmem, smem, smem, smem, vmem, smem, smem],
        out_specs=(anywhere, vmem),
        scratch_shapes=[
            pltpu.VMEM((occ, n_aux, aux_dev, osv), bf16),
            pltpu.VMEM((occ, fit, fit), bf16),
            pltpu.VMEM((occ, aux_total, fit), bf16),
            pltpu.VMEM((aux_total, fit), bf16),
            pltpu.VMEM((occ, fit, aux_total), bf16),
            pltpu.VMEM((occ, 8, aux_total), f32),
            pltpu.VMEM((occ * osv, aux_total), bf16),
            pltpu.VMEM((occ, n_orb, fit, osv), bf16),
            pltpu.VMEM((n_orb, occ, fit), jnp.int32),
            pltpu.VMEM((n_orb, occ, osv), f32),
            pltpu.VMEM((occ * osv, osv), f32),
            pltpu.VMEM((aux_total, occ * n_orb * osv), bf16),
            pltpu.VMEM((occ * osv, n_orb * osv), f32),
            pltpu.VMEM((occ * osv, occ * n_orb * osv), bf16),
            pltpu.VMEM((n_aux, occ, aux_dev, osv), bf16),
            dma((occ, n_aux)),
            dma((occ, n_aux)),
            dma((occ, n_orb)),
            dma((occ, n_orb)),
            dma((2, n_orb)),
            dma((2, n_orb)),
            dma((n_aux,)),
            dma((n_aux,)),
            dma((3,)),
        ],
        compiler_params=pltpu.CompilerParams(
            collective_id=0, has_side_effects=True, vmem_limit_bytes=60 * 1024 * 1024
        ),
    )(
        raw_rows.reshape(n_aux, occ, aux_dev, osv),
        fit_metric,
        domain.reshape(n_aux, occ, fit),
        counts.reshape(-1),
        orbital_ids,
        occ_energy,
        osv_energy,
        matchings.reshape(-1),
        screening.reshape(-1),
    )
    density = returned.reshape(group_slots, aux_dev, osv).astype(f32)
    sums = jnp.sum(sums, axis=3)
    partner = lax.dynamic_index_in_dim(matchings, my_orb, 1, keepdims=False)
    step = jnp.concatenate([jnp.zeros((1,), jnp.int32), lax.rem(my_orb - partner + n_orb, n_orb)])
    chosen = step[:, None] == jnp.arange(n_orb, dtype=jnp.int32)[None, :]
    picked = jnp.sum(
        jnp.where(chosen[None, :, None, :], sums.transpose(2, 0, 1)[:, None, :, :], 0.0), axis=3
    )
    energy = PAIR_SCALE * screening.astype(f32) * picked / (osv * osv)
    return (density, energy)


def solution(mesh):
    placed = (
        P("orb", "aux", None),
        P(("orb", "aux"), None, None),
        P("orb", None),
        P("orb", None),
        P(("orb", "aux")),
        P(),
        P(("orb", "aux"), None),
        P(),
        P(("orb", "aux"), None, None),
    )
    return jax.shard_map(
        per_device,
        mesh=mesh,
        in_specs=placed,
        out_specs=(P("orb", "aux", None), P(("orb", "aux"), None, None)),
        check_vma=False,
    )
```

```python
import functools

import jax
import jax.numpy as jnp
from jax import lax
from jax.experimental import pallas as pl
from jax.experimental.pallas import tpu as pltpu
from jax.sharding import PartitionSpec as P

PAIR_SCALE = 1.3
MESH = pl.DeviceIdType.MESH
NT = (((1,), (1,)), ((), ()))


def kernel(
    n_orb,
    n_aux,
    raw_ref,
    metric_ref,
    domain_ref,
    counts_ref,
    ids_ref,
    occ_ref,
    osv_ref,
    match_ref,
    screen_ref,
    out_ref,
    energy_ref,
    raw_full,
    metric,
    st_own,
    st_far,
    ms,
    rt,
    fitted,
    rows,
    levels,
    level_col,
    grid_full,
    integrals,
    amps,
    outgoing,
    sums,
    totals,
    raw_send,
    raw_recv,
    fit_send,
    fit_recv,
    meta_send,
    meta_recv,
    den_send,
    den_recv,
    local_sem,
):
    occ, fit = metric_ref.shape[0], metric_ref.shape[1]
    aux_dev, osv = raw_ref.shape[2], raw_ref.shape[3]
    aux_total = n_aux * aux_dev
    matches = match_ref.shape[0]
    my_orb = lax.axis_index("orb")
    me = lax.axis_index("aux")

    def aux_peer(step):
        return lax.rem(me + step, n_aux)

    def orb_peer(step):
        return lax.rem(my_orb + step, n_orb)

    barrier = pltpu.get_barrier_semaphore()
    for step in range(1, n_aux):
        pl.semaphore_signal(barrier, inc=1, device_id=(my_orb, aux_peer(step)), device_id_type=MESH)
    for step in range(1, n_orb):
        pl.semaphore_signal(barrier, inc=1, device_id=(orb_peer(step), me), device_id_type=MESH)

    def metric_copy(k):
        return pltpu.make_async_copy(metric_ref.at[k], metric.at[k], local_sem.at[0, k])

    def own_raw(k):
        return pltpu.make_async_copy(raw_ref.at[me, k], raw_full.at[k, me], local_sem.at[1, k])

    for k in range(occ):
        metric_copy(k).start()
        own_raw(k).start()
    pl.semaphore_wait(barrier, n_aux + n_orb - 2)

    def raw_copy(k, step):
        return pltpu.make_async_remote_copy(
            src_ref=raw_ref.at[aux_peer(step), k],
            dst_ref=raw_full.at[k, me],
            send_sem=raw_send.at[k, step],
            recv_sem=raw_recv.at[k, step],
            device_id=(my_orb, aux_peer(step)),
            device_id_type=MESH,
        )

    def fit_copy(k, step):
        return pltpu.make_async_remote_copy(
            src_ref=fitted.at[k, 0],
            dst_ref=fitted.at[k, step],
            send_sem=fit_send.at[k, step],
            recv_sem=fit_recv.at[k, step],
            device_id=(orb_peer(step), me),
            device_id_type=MESH,
        )

    def meta_copy(which, ref, step):
        return pltpu.make_async_remote_copy(
            src_ref=ref.at[0],
            dst_ref=ref.at[step],
            send_sem=meta_send.at[which, step],
            recv_sem=meta_recv.at[which, step],
            device_id=(orb_peer(step), me),
            device_id_type=MESH,
        )

    def den_copy(owner):
        return pltpu.make_async_remote_copy(
            src_ref=outgoing.at[owner],
            dst_ref=out_ref.at[me],
            send_sem=den_send.at[owner],
            recv_sem=den_recv.at[lax.rem(me - owner + n_aux, n_aux)],
            device_id=(my_orb, owner),
            device_id_type=MESH,
        )

    def send_raw(k, carry):
        def one(step, inner):
            raw_copy(k, step).start()
            return inner

        return lax.fori_loop(1, n_aux, one, carry)

    lax.fori_loop(0, occ, send_raw, 0)

    positions = lax.broadcasted_iota(jnp.int32, (1, fit), 1)
    for k in range(occ):
        end = jnp.int32(0)
        owner = jnp.zeros((1, fit), jnp.int32)
        for j in range(n_aux):
            end = end + counts_ref[j, me * occ + k]
            owner = owner + jnp.where(positions >= end, 1, 0)
        rows[0, k : k + 1, :] = owner * aux_dev + domain_ref[pl.ds(me * occ + k, 1), :]
        level = osv_ref[k : k + 1, :].astype(jnp.float32) - occ_ref[ids_ref[k]]
        levels[0, k : k + 1, :] = level
        level_col[k * osv : (k + 1) * osv, :] = jnp.broadcast_to(level, (osv, osv)).T
    for step in range(1, n_orb):
        meta_copy(0, rows, step).start()
        meta_copy(1, levels, step).start()

    def place(row, target):
        height = 128
        base = lax.broadcasted_iota(jnp.int32, (height, fit), 0).astype(jnp.bfloat16)
        one, zero = jnp.ones((), jnp.bfloat16), jnp.zeros((), jnp.bfloat16)
        for j in range(aux_total // height):
            inside = jnp.logical_and(row >= j * height, row < (j + 1) * height)
            wanted = jnp.where(inside, row - j * height, -1).astype(jnp.bfloat16)
            target[j * height : (j + 1) * height, :] = jnp.where(base == wanted, one, zero)

    def lanes(l, step):
        return pl.ds(pl.multiple_of((l * n_orb + step) * osv, osv), osv)

    ones = jnp.ones((8, fit), jnp.bfloat16)

    def place_far(l):
        def one(step, inner):
            place(rows[step, pl.ds(l, 1), :], st_far.at[step - 1])
            return inner

        lax.fori_loop(1, n_orb, one, 0)

    def spread_far(l):
        def one(step, inner):
            fit_copy(l, step).wait_recv()
            grid_full[:, lanes(l, step)] = jnp.dot(
                st_far[step - 1], fitted[l, step], preferred_element_type=jnp.float32
            ).astype(jnp.bfloat16)
            return inner

        lax.fori_loop(1, n_orb, one, 0)

    def fit_own(k, carry):
        place(rows[0, pl.ds(k, 1), :], st_own)
        metric_copy(k).wait()
        ms[...] = lax.dot_general(
            metric[k], st_own[...], NT, preferred_element_type=jnp.float32
        ).astype(jnp.bfloat16)
        mask = lax.dot_general(ones, st_own[...], NT, preferred_element_type=jnp.float32)

        def arrived(step, inner):
            raw_copy(k, step).wait_recv()
            return inner

        lax.fori_loop(1, n_aux, arrived, 0)
        own_raw(k).wait()
        dense = raw_full[k].reshape(aux_total, osv)
        block = jnp.dot(ms[...], dense, preferred_element_type=jnp.float32).astype(jnp.bfloat16)
        fitted[k, 0] = block
        for step in range(1, n_orb):
            fit_copy(k, step).start()
        rt[pl.ds(pl.multiple_of(k * osv, osv), osv), :] = jnp.where(
            mask[0:1, :] > 0.5, dense.astype(jnp.float32).T, 0.0
        ).astype(jnp.bfloat16)
        grid_full[:, lanes(k, 0)] = jnp.dot(
            st_own[...], block, preferred_element_type=jnp.float32
        ).astype(jnp.bfloat16)

        @pl.when(k == 0)
        def _():
            for step in range(1, n_orb):
                meta_copy(0, rows, step).wait_recv()
                meta_copy(1, levels, step).wait_recv()

        @pl.when(k > 0)
        def _():
            spread_far(k - 1)

        place_far(k)
        return carry

    lax.fori_loop(0, occ, fit_own, 0)

    def partners(l, carry):
        @pl.when(l == occ - 1)
        def _():
            spread_far(l)

        wide = n_orb * osv
        part = pl.ds(pl.multiple_of(l * wide, wide), wide)
        integrals[...] = jnp.dot(rt[...], grid_full[:, part], preferred_element_type=jnp.float32)

        def terms(step, inner):
            far = levels[step, pl.ds(l, 1), :]
            peer = lax.rem(my_orb - step + n_orb, n_orb)
            local = pl.ds(pl.multiple_of(step * osv, osv), osv)
            for k in range(occ):
                weight = jnp.where(step == 0, screen_ref[k, l, 0], 0)
                for q in range(matches):
                    weight = weight + jnp.where(
                        jnp.logical_and(step > 0, match_ref[q, my_orb] == peer),
                        screen_ref[k, l, q + 1],
                        0,
                    )
                value = integrals[k * osv : (k + 1) * osv, local]
                bottom = level_col[k * osv : (k + 1) * osv, :] + far
                amp = (value / bottom).astype(jnp.bfloat16).astype(jnp.float32)
                sums[l, step, k : k + 1, :] = jnp.sum(amp * value, axis=0, keepdims=True)
                amps[k * osv : (k + 1) * osv, lanes(l, step)] = (
                    amp * weight.astype(jnp.float32)
                ).astype(jnp.bfloat16)
            return inner

        return lax.fori_loop(0, n_orb, terms, carry)

    lax.fori_loop(0, occ, partners, 0)

    pair = 2
    my_pair = me // pair

    def density(which):
        height = pair * aux_dev
        part = grid_full[pl.ds(pl.multiple_of(which * height, height), height), :]
        found = lax.dot_general(part, amps[...], NT, preferred_element_type=jnp.float32)
        found = found.astype(jnp.bfloat16)
        for c in range(pair):
            for k in range(occ):
                outgoing[which * pair + c, k] = found[
                    c * aux_dev : (c + 1) * aux_dev, k * osv : (k + 1) * osv
                ]

    def far_density(step, carry):
        which = lax.rem(my_pair + step, n_aux // pair)
        density(which)
        for c in range(pair):
            den_copy(which * pair + c).start()
        return carry

    lax.fori_loop(1, n_aux // pair, far_density, 0)
    density(my_pair)
    buddy = my_pair * pair + 1 - lax.rem(me, pair)
    den_copy(buddy).start()
    own_out = pltpu.make_async_copy(outgoing.at[me], out_ref.at[me], local_sem.at[2, 0])
    own_out.start()

    def energies(l, carry):
        for k in range(occ):
            for step in range(n_orb):
                totals[step] = jnp.sum(sums[l, step, k : k + 1, :]) * (PAIR_SCALE / (osv * osv))
            energy_ref[k, l, 0] = screen_ref[k, l, 0].astype(jnp.float32) * totals[0]
            for q in range(matches):
                found = jnp.float32(0.0)
                for step in range(1, n_orb):
                    peer = lax.rem(my_orb - step + n_orb, n_orb)
                    found = jnp.where(match_ref[q, my_orb] == peer, totals[step], found)
                energy_ref[k, l, q + 1] = screen_ref[k, l, q + 1].astype(jnp.float32) * found
        return carry

    lax.fori_loop(0, occ, energies, 0)

    def drain_raw(k, carry):
        def one(step, inner):
            raw_copy(k, step).wait_send()
            return inner

        lax.fori_loop(1, n_aux, one, 0)

        def two(step, inner):
            fit_copy(k, step).wait_send()
            return inner

        return lax.fori_loop(1, n_orb, two, carry)

    lax.fori_loop(0, occ, drain_raw, 0)
    for step in range(1, n_orb):
        meta_copy(0, rows, step).wait_send()
        meta_copy(1, levels, step).wait_send()

    def drain_density(step, carry):
        copy = den_copy(aux_peer(step))
        copy.wait_send()
        copy.wait_recv()
        return carry

    lax.fori_loop(1, n_aux, drain_density, 0)
    own_out.wait()


def per_device(
    raw_rows, fit_metric, domain, counts, orbital_ids, occ_energy, osv_energy, matchings, screening
):
    n_aux = lax.axis_size("aux")
    n_orb = lax.axis_size("orb")
    group_slots, aux_dev, osv = raw_rows.shape
    occ = group_slots // n_aux
    fit = domain.shape[1]
    aux_total = aux_dev * n_aux
    bf16, f32 = jnp.bfloat16, jnp.float32
    anywhere = pl.BlockSpec(memory_space=pl.ANY)
    vmem = pl.BlockSpec(memory_space=pltpu.VMEM)
    smem = pl.BlockSpec(memory_space=pltpu.SMEM)
    dma = pltpu.SemaphoreType.DMA
    returned, energy = pl.pallas_call(
        functools.partial(kernel, n_orb, n_aux),
        out_shape=(
            jax.ShapeDtypeStruct((n_aux, occ, aux_dev, osv), bf16),
            jax.ShapeDtypeStruct((occ, occ, screening.shape[1]), f32),
        ),
        in_specs=[anywhere, anywhere, vmem, smem, smem, smem, vmem, smem, smem],
        out_specs=(anywhere, smem),
        scratch_shapes=[
            pltpu.VMEM((occ, n_aux, aux_dev, osv), bf16),
            pltpu.VMEM((occ, fit, fit), bf16),
            pltpu.VMEM((aux_total, fit), bf16),
            pltpu.VMEM((n_orb - 1, aux_total, fit), bf16),
            pltpu.VMEM((fit, aux_total), bf16),
            pltpu.VMEM((occ * osv, aux_total), bf16),
            pltpu.VMEM((occ, n_orb, fit, osv), bf16),
            pltpu.VMEM((n_orb, occ, fit), jnp.int32),
            pltpu.VMEM((n_orb, occ, osv), f32),
            pltpu.VMEM((occ * osv, osv), f32),
            pltpu.VMEM((aux_total, occ * n_orb * osv), bf16),
            pltpu.VMEM((occ * osv, n_orb * osv), f32),
            pltpu.VMEM((occ * osv, occ * n_orb * osv), bf16),
            pltpu.VMEM((n_aux, occ, aux_dev, osv), bf16),
            pltpu.VMEM((occ, n_orb, occ, osv), f32),
            pltpu.SMEM((n_orb,), f32),
            dma((occ, n_aux)),
            dma((occ, n_aux)),
            dma((occ, n_orb)),
            dma((occ, n_orb)),
            dma((2, n_orb)),
            dma((2, n_orb)),
            dma((n_aux,)),
            dma((n_aux,)),
            dma((3, occ)),
        ],
        compiler_params=pltpu.CompilerParams(
            collective_id=0, has_side_effects=True, vmem_limit_bytes=56 * 1024 * 1024
        ),
    )(
        raw_rows.reshape(n_aux, occ, aux_dev, osv),
        fit_metric,
        domain,
        counts.T,
        orbital_ids,
        occ_energy,
        osv_energy,
        matchings,
        screening.transpose(0, 2, 1),
    )
    density = returned.reshape(group_slots, aux_dev, osv).astype(f32)
    return (density, energy.transpose(0, 2, 1))


def solution(mesh):
    placed = (
        P("orb", "aux", None),
        P(("orb", "aux"), None, None),
        P("orb", None),
        P("orb", None),
        P(("orb", "aux")),
        P(),
        P(("orb", "aux"), None),
        P(),
        P(("orb", "aux"), None, None),
    )
    return jax.shard_map(
        per_device,
        mesh=mesh,
        in_specs=placed,
        out_specs=(P("orb", "aux", None), P(("orb", "aux"), None, None)),
        check_vma=False,
    )
```

```python
import functools

import jax
import jax.numpy as jnp
from jax import lax
from jax.experimental import pallas as pl
from jax.experimental.pallas import tpu as pltpu
from jax.sharding import PartitionSpec as P

PAIR_SCALE = 1.3
MESH = pl.DeviceIdType.MESH
NT = (((1,), (1,)), ((), ()))


def kernel(
    n_orb,
    n_aux,
    raw_ref,
    metric_ref,
    domain_ref,
    counts_ref,
    ids_ref,
    occ_ref,
    osv_ref,
    match_ref,
    screen_ref,
    out_ref,
    energy_ref,
    raw_full,
    metric,
    st_own,
    st_far,
    ms,
    rt,
    fitted,
    rows,
    levels,
    level_col,
    grid_full,
    integrals,
    amps,
    outgoing,
    sums,
    totals,
    raw_send,
    raw_recv,
    fit_send,
    fit_recv,
    meta_send,
    meta_recv,
    den_send,
    den_recv,
    local_sem,
):
    occ, fit = metric_ref.shape[0], metric_ref.shape[1]
    aux_dev, osv = raw_ref.shape[2], raw_ref.shape[3]
    aux_total = n_aux * aux_dev
    matches = match_ref.shape[0]
    my_orb = lax.axis_index("orb")
    me = lax.axis_index("aux")

    def aux_peer(step):
        return lax.rem(me + step, n_aux)

    def orb_peer(step):
        return lax.rem(my_orb + step, n_orb)

    barrier = pltpu.get_barrier_semaphore()
    for step in range(1, n_aux):
        pl.semaphore_signal(barrier, inc=1, device_id=(my_orb, aux_peer(step)), device_id_type=MESH)
    for step in range(1, n_orb):
        pl.semaphore_signal(barrier, inc=1, device_id=(orb_peer(step), me), device_id_type=MESH)

    def metric_copy(k):
        return pltpu.make_async_copy(metric_ref.at[k], metric.at[k], local_sem.at[0, k])

    def own_raw(k):
        return pltpu.make_async_copy(raw_ref.at[me, k], raw_full.at[k, me], local_sem.at[1, k])

    for k in range(occ):
        metric_copy(k).start()
        own_raw(k).start()
    pl.semaphore_wait(barrier, n_aux + n_orb - 2)

    def raw_copy(k, step):
        return pltpu.make_async_remote_copy(
            src_ref=raw_ref.at[aux_peer(step), k],
            dst_ref=raw_full.at[k, me],
            send_sem=raw_send.at[k, step],
            recv_sem=raw_recv.at[k, step],
            device_id=(my_orb, aux_peer(step)),
            device_id_type=MESH,
        )

    def fit_copy(k, step):
        return pltpu.make_async_remote_copy(
            src_ref=fitted.at[k, 0],
            dst_ref=fitted.at[k, step],
            send_sem=fit_send.at[k, step],
            recv_sem=fit_recv.at[k, step],
            device_id=(orb_peer(step), me),
            device_id_type=MESH,
        )

    def meta_copy(which, ref, step):
        return pltpu.make_async_remote_copy(
            src_ref=ref.at[0],
            dst_ref=ref.at[step],
            send_sem=meta_send.at[which, step],
            recv_sem=meta_recv.at[which, step],
            device_id=(orb_peer(step), me),
            device_id_type=MESH,
        )

    def den_copy(owner):
        return pltpu.make_async_remote_copy(
            src_ref=outgoing.at[owner],
            dst_ref=out_ref.at[me],
            send_sem=den_send.at[owner],
            recv_sem=den_recv.at[lax.rem(me - owner + n_aux, n_aux)],
            device_id=(my_orb, owner),
            device_id_type=MESH,
        )

    def send_raw(k, carry):
        def one(step, inner):
            raw_copy(k, step).start()
            return inner

        return lax.fori_loop(1, n_aux, one, carry)

    lax.fori_loop(0, occ, send_raw, 0)

    positions = lax.broadcasted_iota(jnp.int32, (1, fit), 1)
    for k in range(occ):
        end = jnp.int32(0)
        owner = jnp.zeros((1, fit), jnp.int32)
        for j in range(n_aux):
            end = end + counts_ref[j, me * occ + k]
            owner = owner + jnp.where(positions >= end, 1, 0)
        rows[0, k : k + 1, :] = owner * aux_dev + domain_ref[pl.ds(me * occ + k, 1), :]
        level = osv_ref[k : k + 1, :].astype(jnp.float32) - occ_ref[ids_ref[k]]
        levels[0, k : k + 1, :] = level
        level_col[k * osv : (k + 1) * osv, :] = jnp.broadcast_to(level, (osv, osv)).T
    for step in range(1, n_orb):
        meta_copy(0, rows, step).start()
        meta_copy(1, levels, step).start()

    def place(row, target):
        height = 128
        base = lax.broadcasted_iota(jnp.int32, (height, fit), 0).astype(jnp.bfloat16)
        one, zero = jnp.ones((), jnp.bfloat16), jnp.zeros((), jnp.bfloat16)
        for j in range(aux_total // height):
            inside = jnp.logical_and(row >= j * height, row < (j + 1) * height)
            wanted = jnp.where(inside, row - j * height, -1).astype(jnp.bfloat16)
            target[j * height : (j + 1) * height, :] = jnp.where(base == wanted, one, zero)

    def lanes(l, step):
        return pl.ds(pl.multiple_of((l * n_orb + step) * osv, osv), osv)

    ones = jnp.ones((8, fit), jnp.bfloat16)

    def place_far(l):
        def one(step, inner):
            place(rows[step, pl.ds(l, 1), :], st_far.at[step - 1])
            return inner

        lax.fori_loop(1, n_orb, one, 0)

    def spread_far(l):
        def one(step, inner):
            fit_copy(l, step).wait_recv()
            grid_full[:, lanes(l, step)] = jnp.dot(
                st_far[step - 1], fitted[l, step], preferred_element_type=jnp.float32
            ).astype(jnp.bfloat16)
            return inner

        lax.fori_loop(1, n_orb, one, 0)

    def fit_own(k, carry):
        place(rows[0, pl.ds(k, 1), :], st_own)
        metric_copy(k).wait()
        ms[...] = lax.dot_general(
            metric[k], st_own[...], NT, preferred_element_type=jnp.float32
        ).astype(jnp.bfloat16)
        mask = lax.dot_general(ones, st_own[...], NT, preferred_element_type=jnp.float32)

        def arrived(step, inner):
            raw_copy(k, step).wait_recv()
            return inner

        lax.fori_loop(1, n_aux, arrived, 0)
        own_raw(k).wait()
        dense = raw_full[k].reshape(aux_total, osv)
        block = jnp.dot(ms[...], dense, preferred_element_type=jnp.float32).astype(jnp.bfloat16)
        fitted[k, 0] = block
        for step in range(1, n_orb):
            fit_copy(k, step).start()
        rt[pl.ds(pl.multiple_of(k * osv, osv), osv), :] = jnp.where(
            mask[0:1, :] > 0.5, dense.astype(jnp.float32).T, 0.0
        ).astype(jnp.bfloat16)
        grid_full[:, lanes(k, 0)] = jnp.dot(
            st_own[...], block, preferred_element_type=jnp.float32
        ).astype(jnp.bfloat16)

        @pl.when(k == 0)
        def _():
            for step in range(1, n_orb):
                meta_copy(0, rows, step).wait_recv()
                meta_copy(1, levels, step).wait_recv()

        @pl.when(k > 0)
        def _():
            spread_far(k - 1)

        place_far(k)
        return carry

    lax.fori_loop(0, occ, fit_own, 0)

    def partners(l, carry):
        @pl.when(l == occ - 1)
        def _():
            spread_far(l)

        wide = n_orb * osv
        part = pl.ds(pl.multiple_of(l * wide, wide), wide)
        integrals[...] = jnp.dot(rt[...], grid_full[:, part], preferred_element_type=jnp.float32)

        def terms(step, inner):
            far = levels[step, pl.ds(l, 1), :]
            peer = lax.rem(my_orb - step + n_orb, n_orb)
            local = pl.ds(pl.multiple_of(step * osv, osv), osv)
            for k in range(occ):
                weight = jnp.where(step == 0, screen_ref[k, l, 0], 0)
                for q in range(matches):
                    weight = weight + jnp.where(
                        jnp.logical_and(step > 0, match_ref[q, my_orb] == peer),
                        screen_ref[k, l, q + 1],
                        0,
                    )
                value = integrals[k * osv : (k + 1) * osv, local]
                bottom = level_col[k * osv : (k + 1) * osv, :] + far
                amp = (value / bottom).astype(jnp.bfloat16).astype(jnp.float32)
                sums[l, step, k : k + 1, :] = jnp.sum(amp * value, axis=0, keepdims=True)
                amps[k * osv : (k + 1) * osv, lanes(l, step)] = (
                    amp * weight.astype(jnp.float32)
                ).astype(jnp.bfloat16)
            return inner

        return lax.fori_loop(0, n_orb, terms, carry)

    lax.fori_loop(0, occ, partners, 0)

    pair = 2
    my_pair = me // pair

    def density(which):
        height = pair * aux_dev
        part = grid_full[pl.ds(pl.multiple_of(which * height, height), height), :]
        found = lax.dot_general(part, amps[...], NT, preferred_element_type=jnp.float32)
        found = found.astype(jnp.bfloat16)
        for c in range(pair):
            for k in range(occ):
                outgoing[which * pair + c, k] = found[
                    c * aux_dev : (c + 1) * aux_dev, k * osv : (k + 1) * osv
                ]

    def far_density(step, carry):
        which = lax.rem(my_pair + n_aux // pair - step, n_aux // pair)
        density(which)
        for c in range(pair):
            den_copy(which * pair + c).start()
        return carry

    lax.fori_loop(1, n_aux // pair, far_density, 0)
    density(my_pair)
    buddy = my_pair * pair + 1 - lax.rem(me, pair)
    den_copy(buddy).start()
    own_out = pltpu.make_async_copy(outgoing.at[me], out_ref.at[me], local_sem.at[2, 0])
    own_out.start()

    def energies(l, carry):
        for k in range(occ):
            for step in range(n_orb):
                totals[step] = jnp.sum(sums[l, step, k : k + 1, :]) * (PAIR_SCALE / (osv * osv))
            energy_ref[k, l, 0] = screen_ref[k, l, 0].astype(jnp.float32) * totals[0]
            for q in range(matches):
                found = jnp.float32(0.0)
                for step in range(1, n_orb):
                    peer = lax.rem(my_orb - step + n_orb, n_orb)
                    found = jnp.where(match_ref[q, my_orb] == peer, totals[step], found)
                energy_ref[k, l, q + 1] = screen_ref[k, l, q + 1].astype(jnp.float32) * found
        return carry

    lax.fori_loop(0, occ, energies, 0)

    def drain_raw(k, carry):
        def one(step, inner):
            raw_copy(k, step).wait_send()
            return inner

        lax.fori_loop(1, n_aux, one, 0)

        def two(step, inner):
            fit_copy(k, step).wait_send()
            return inner

        return lax.fori_loop(1, n_orb, two, carry)

    lax.fori_loop(0, occ, drain_raw, 0)
    for step in range(1, n_orb):
        meta_copy(0, rows, step).wait_send()
        meta_copy(1, levels, step).wait_send()

    def drain_density(step, carry):
        copy = den_copy(aux_peer(step))
        copy.wait_send()
        copy.wait_recv()
        return carry

    lax.fori_loop(1, n_aux, drain_density, 0)
    own_out.wait()


def per_device(
    raw_rows, fit_metric, domain, counts, orbital_ids, occ_energy, osv_energy, matchings, screening
):
    n_aux = lax.axis_size("aux")
    n_orb = lax.axis_size("orb")
    group_slots, aux_dev, osv = raw_rows.shape
    occ = group_slots // n_aux
    fit = domain.shape[1]
    aux_total = aux_dev * n_aux
    bf16, f32 = jnp.bfloat16, jnp.float32
    anywhere = pl.BlockSpec(memory_space=pl.ANY)
    vmem = pl.BlockSpec(memory_space=pltpu.VMEM)
    smem = pl.BlockSpec(memory_space=pltpu.SMEM)
    dma = pltpu.SemaphoreType.DMA
    returned, energy = pl.pallas_call(
        functools.partial(kernel, n_orb, n_aux),
        out_shape=(
            jax.ShapeDtypeStruct((n_aux, occ, aux_dev, osv), bf16),
            jax.ShapeDtypeStruct((occ, occ, screening.shape[1]), f32),
        ),
        in_specs=[anywhere, anywhere, vmem, smem, smem, smem, vmem, smem, smem],
        out_specs=(anywhere, smem),
        scratch_shapes=[
            pltpu.VMEM((occ, n_aux, aux_dev, osv), bf16),
            pltpu.VMEM((occ, fit, fit), bf16),
            pltpu.VMEM((aux_total, fit), bf16),
            pltpu.VMEM((n_orb - 1, aux_total, fit), bf16),
            pltpu.VMEM((fit, aux_total), bf16),
            pltpu.VMEM((occ * osv, aux_total), bf16),
            pltpu.VMEM((occ, n_orb, fit, osv), bf16),
            pltpu.VMEM((n_orb, occ, fit), jnp.int32),
            pltpu.VMEM((n_orb, occ, osv), f32),
            pltpu.VMEM((occ * osv, osv), f32),
            pltpu.VMEM((aux_total, occ * n_orb * osv), bf16),
            pltpu.VMEM((occ * osv, n_orb * osv), f32),
            pltpu.VMEM((occ * osv, occ * n_orb * osv), bf16),
            pltpu.VMEM((n_aux, occ, aux_dev, osv), bf16),
            pltpu.VMEM((occ, n_orb, occ, osv), f32),
            pltpu.SMEM((n_orb,), f32),
            dma((occ, n_aux)),
            dma((occ, n_aux)),
            dma((occ, n_orb)),
            dma((occ, n_orb)),
            dma((2, n_orb)),
            dma((2, n_orb)),
            dma((n_aux,)),
            dma((n_aux,)),
            dma((3, occ)),
        ],
        compiler_params=pltpu.CompilerParams(
            collective_id=0, has_side_effects=True, vmem_limit_bytes=56 * 1024 * 1024
        ),
    )(
        raw_rows.reshape(n_aux, occ, aux_dev, osv),
        fit_metric,
        domain,
        counts.T,
        orbital_ids,
        occ_energy,
        osv_energy,
        matchings,
        screening.transpose(0, 2, 1),
    )
    density = returned.reshape(group_slots, aux_dev, osv).astype(f32)
    return (density, energy.transpose(0, 2, 1))


def solution(mesh):
    placed = (
        P("orb", "aux", None),
        P(("orb", "aux"), None, None),
        P("orb", None),
        P("orb", None),
        P(("orb", "aux")),
        P(),
        P(("orb", "aux"), None),
        P(),
        P(("orb", "aux"), None, None),
    )
    return jax.shard_map(
        per_device,
        mesh=mesh,
        in_specs=placed,
        out_specs=(P("orb", "aux", None), P(("orb", "aux"), None, None)),
        check_vma=False,
    )
```
